32 devices in a mesh: band: 16 (over z, x, core), ga: 2 (over y).
Axes of the slice: x: 2, y: 2, z: 4, core: 2. Of those that a mesh axis runs over, the one named last changes fastest.
Arguments:
- psi: float32 [2, 4096, 65536], P(None, 'band', 'ga'), may hold values from -0.0234375 to 0.0234375
- hx: float32 [2, 256, 65536], P(None, 'band', 'ga'), may hold values from -6 to 6
Outputs:
- h_sub: float32 [2, 4096, 256], P(None, ('band', 'ga'))
The draws below stay inside these ranges and needn't reach their ends.
All inputs are finite; a program needn't handle non-finite values.
Results may differ from the reference program's by a relative error of at most 0.00007.
Values sent between devices are 32-bit elements; how exact they have to be, the bound alone decides.
A program may use at most 192 MiB of HBM per device.

```python
import jax
import jax.numpy as jnp
from jax import lax

NB = 4096
NG = 65536
NBLK = 256


def level_of(stream_key, dims, shards, smallest, high):
    def one(position, shards_of):
        draws = jax.random.uniform(jax.random.fold_in(jax.random.fold_in(stream_key, 6), position), (shards_of,), jnp.float32, smallest / len(shards), high / len(shards))
        return jnp.repeat(jnp.exp(draws), dims[position] // shards_of).reshape((-1,) + (1,) * (len(dims) - position - 1))

    gain = one(*shards[0])
    for cut in shards[1:]:
        gain = gain * one(*cut)
    return gain


def gaussian(key, extent, scale, reach, split=(), held_as=jnp.bfloat16):
    factor_of = level_of(key, extent, split, -0.22, 0.18) if split else 1.0
    entries = jax.random.normal(key, extent, jnp.float32) * scale * factor_of
    return jnp.minimum(jnp.maximum(entries, -reach), reach).astype(held_as)


def setup_inputs(seed: int = 0) -> dict:
    key_list = jax.random.split(jax.random.key(seed), 3)
    psi = gaussian(key_list[0], (2, NB, NG), NG ** -0.5, 0.0234375, ((1, 16), (2, 2)), jnp.float32)
    hx = gaussian(key_list[1], (2, NBLK, NG), 1.0, 6.0, ((1, 16), (2, 2)), jnp.float32)
    return dict(psi=psi, hx=hx)


def contract(left, right):
    return lax.dot_general(left, right, (((1,), (1,)), ((), ())), precision=lax.Precision.HIGHEST, preferred_element_type=jnp.float32)


def reference(psi, hx):
    real_part = contract(psi[0], hx[0]) + contract(psi[1], hx[1])
    imag_part = contract(psi[0], hx[1]) - contract(psi[1], hx[0])
    return jnp.stack([real_part, imag_part], axis=0)
```

```python
import functools

import jax
import jax.numpy as jnp
from jax import lax
from jax.experimental import pallas as pl
from jax.experimental.pallas import tpu as pltpu
from jax.sharding import PartitionSpec as P

CHUNKS = 8
TILE = 512
SLOTS = 3
MESH = pl.DeviceIdType.MESH


def ladder(mesh):
    chips = mesh.shape["band"] // 2
    try:
        coords = [tuple(mesh.devices[2 * j, 0].coords) for j in range(chips)]
    except AttributeError:
        return 1, 2
    axis = [a != b for a, b in zip(coords[0], coords[1])].index(True)
    if len({c[axis] for c in coords}) == 2:
        return 1, 2
    return chips // 2, 1


def split(x):
    high = x.astype(jnp.bfloat16)
    low = (x - high.astype(jnp.float32)).astype(jnp.bfloat16)
    return high, low


def kernel(
    chips,
    owners,
    strides,
    psi,
    hx,
    out,
    ring,
    twin,
    psi_v,
    hx_v,
    acc,
    final,
    others,
    ring_send,
    ring_recv,
    twin_send,
    twin_recv,
    psi_sem,
    own_sem,
    twin_sem,
    y_send,
    y_recv,
):
    depth = hx.shape[-1]
    half = depth // 2
    width = half // CHUNKS
    rows = psi.shape[1]
    height = rows // owners
    mid = chips // 2
    ticks = chips * CHUNKS
    vectors = hx.shape[1]
    x_stride, z_stride = strides
    long = mid

    me = lax.axis_index("band")
    y = lax.axis_index("ga")
    core = lax.rem(me, 2)
    chip = me // 2
    x = lax.rem(chip // x_stride, 2)
    z = lax.rem(chip // z_stride, long)
    place = z + x * (2 * long - 1 - 2 * z)

    def device_at(position):
        at_x = position // long
        at_z = position + at_x * (2 * long - 1 - 2 * position)
        return 2 * (at_x * x_stride + at_z * z_stride) + core

    after = device_at(lax.rem(place + 1, chips))
    before = device_at(lax.rem(place + chips - 1, chips))
    partner = me + 1 - 2 * core
    target = (after, before)

    def columns(way, c):
        return pl.ds(pl.multiple_of(way * half + c * width, 128), width)

    def with_held(step, way, c, act):
        cols = columns(way, c)
        if isinstance(step, int):
            act(hx.at[:, :, cols] if step == 0 else ring.at[step - 1, :, :, cols])
            return
        pl.when(step == 0)(lambda: act(hx.at[:, :, cols]))
        pl.when(step > 0)(lambda: act(ring.at[step - 1, :, :, cols]))

    def ring_copy(step, way, c, source):
        return pltpu.make_async_remote_copy(
            src_ref=source,
            dst_ref=ring.at[step, :, :, columns(way, c)],
            send_sem=ring_send.at[way, step, c],
            recv_sem=ring_recv.at[way, step, c],
            device_id={"band": target[way]},
            device_id_type=MESH,
        )

    def twin_copy(step, way, c, source):
        return pltpu.make_async_remote_copy(
            src_ref=source,
            dst_ref=twin.at[step, :, :, columns(way, c)],
            send_sem=twin_send.at[way, step, c],
            recv_sem=twin_recv.at[way, step, c],
            device_id={"band": partner},
            device_id_type=MESH,
        )

    def psi_load(t, way):
        c = lax.rem(t, CHUNKS)
        slot = lax.rem(t, SLOTS)
        return pltpu.make_async_copy(
            psi.at[:, :, columns(way, c)], psi_v.at[slot, way], psi_sem.at[slot, way]
        )

    def own_load(t, way, source):
        slot = lax.rem(t, SLOTS)
        return pltpu.make_async_copy(
            source, hx_v.at[slot, way, :, core], own_sem.at[slot, way]
        )

    def twin_load(t, way):
        step, c = t // CHUNKS, lax.rem(t, CHUNKS)
        slot = lax.rem(t, SLOTS)
        return pltpu.make_async_copy(
            twin.at[step, :, :, columns(way, c)],
            hx_v.at[slot, way, :, 1 - core],
            twin_sem.at[slot, way],
        )

    def place_of(step, way):
        late = step // mid
        pair = (1 - late) * step + late * lax.rem(chips - step, mid)
        side = late if way == 0 else lax.rem((step + mid - 1) // mid, 2)
        return 2 * pair + side

    def compute(t, way):
        step, c = t // CHUNKS, lax.rem(t, CHUNKS)
        slot = lax.rem(t, SLOTS)
        own_load(t, way, hx.at[:, :, columns(way, c)]).wait()
        twin_load(t, way).wait()
        psi_load(t, way).wait()
        where = place_of(step, way)
        tile = min(TILE, width)

        def body(k, carry):
            cols = pl.ds(pl.multiple_of(k * tile, 128), tile)
            real = hx_v[slot, way, 0, :, :, cols].reshape(2 * vectors, tile)
            imag = hx_v[slot, way, 1, :, :, cols].reshape(2 * vectors, tile)
            real_high, real_low = split(real)
            imag_high, imag_low = split(imag)
            first = jnp.concatenate([real_high, imag_high, real_low, imag_low], axis=0)
            second = jnp.concatenate(
                [imag_high, -real_high, imag_low, -real_low], axis=0
            )
            total = acc[where]
            for part, right in ((0, first), (1, second)):
                for left in split(psi_v[slot, way, part, :, cols]):
                    total += lax.dot_general(
                        left,
                        right,
                        (((1,), (1,)), ((), ())),
                        preferred_element_type=jnp.float32,
                    )
            acc[where] = total
            return carry

        lax.fori_loop(0, width // tile, body, 0)

    def y_copy(pair, step):
        to = lax.rem(y + step, owners)
        start = pl.multiple_of(to * height, 8)
        return pltpu.make_async_remote_copy(
            src_ref=final.at[pair, pl.ds(start, height)],
            dst_ref=others.at[pair, step - 1],
            send_sem=y_send.at[pair, step - 1],
            recv_sem=y_recv.at[pair, step - 1],
            device_id={"ga": to},
            device_id_type=MESH,
        )

    def finish(step):
        pair = lax.rem(chips - step, mid)
        sides = []
        for side in range(2):
            value = acc[2 * pair + side]
            sides.append(value[:, : 4 * vectors] + value[:, 4 * vectors :])
        final[pair] = jnp.concatenate(sides, axis=1)
        for step_y in range(1, owners):
            y_copy(pair, step_y).start()

    barrier = pltpu.get_barrier_semaphore()
    for neighbour in (after, before, partner):
        pl.semaphore_signal(
            barrier, inc=1, device_id={"band": neighbour}, device_id_type=MESH
        )
    for step_y in range(1, owners):
        pl.semaphore_signal(
            barrier,
            inc=1,
            device_id={"ga": lax.rem(y + step_y, owners)},
            device_id_type=MESH,
        )
    pl.semaphore_wait(barrier, 2 + owners)

    def first_sends(c, carry):
        for way in range(2):
            ring_copy(0, way, c, hx.at[:, :, columns(way, c)]).start()
        return carry

    lax.fori_loop(0, CHUNKS, first_sends, 0)
    acc[...] = jnp.zeros_like(acc)

    def tick(t, carry):
        step, c = t // CHUNKS, lax.rem(t, CHUNKS)

        @pl.when(t < ticks)
        def _():
            for way in range(2):
                psi_load(t, way).start()

        @pl.when(t >= 2)
        def _():
            compute(t - 2, 0)

        @pl.when((t >= 1) & (t <= ticks))
        def _():
            held = t - 1
            held_step, held_c = held // CHUNKS, lax.rem(held, CHUNKS)
            for way in range(2):
                source = hx.at[:, :, columns(way, held_c)]
                twin_copy(held_step, way, held_c, source).wait_recv()
                twin_load(held, way).start()

        @pl.when(t >= 2)
        def _():
            compute(t - 2, 1)
            done = t - 2
            done_step = done // CHUNKS
            pl.when((lax.rem(done, CHUNKS) == CHUNKS - 1) & (done_step >= mid))(
                lambda: finish(done_step)
            )

        @pl.when(t < ticks)
        def _():
            for way in range(2):

                @pl.when(step >= 1)
                def _():
                    source = hx.at[:, :, columns(way, c)]
                    ring_copy(step - 1, way, c, source).wait_recv()

                    @pl.when(step < chips - 1)
                    def _():
                        held = ring.at[step - 1, :, :, columns(way, c)]
                        ring_copy(step, way, c, held).start()

                with_held(
                    step, way, c, lambda ref: twin_copy(step, way, c, ref).start()
                )
                with_held(step, way, c, lambda ref: own_load(t, way, ref).start())

        return carry

    lax.fori_loop(0, ticks + 2, tick, 0)

    def last_waits(t, carry):
        step, c = t // CHUNKS, lax.rem(t, CHUNKS)
        for way in range(2):
            source = hx.at[:, :, columns(way, c)]
            twin_copy(step, way, c, source).wait_send()

            @pl.when(step < chips - 1)
            def _():
                ring_copy(step, way, c, source).wait_send()

        return carry

    lax.fori_loop(0, ticks, last_waits, 0)

    mine = pl.ds(pl.multiple_of(y * height, 8), height)
    for pair in range(mid):
        for step_y in range(1, owners):
            y_copy(pair, step_y).wait_recv()
            final[pair, mine] += others[pair, step_y - 1]
        for step_y in range(1, owners):
            y_copy(pair, step_y).wait_send()

    wide = 2 * vectors
    pieces = [[], []]
    for j in range(chips):
        at_x, at_z = (j // x_stride) % 2, (j // z_stride) % long
        position = at_z + at_x * (2 * long - 1 - 2 * at_z)
        away = lax.rem(place + chips - position, chips)
        late = away // mid
        pair = (1 - late) * away + late * lax.rem(chips - away, mid)
        both = final[pair, mine]
        block = jnp.where(late == 1, both[:, 2 * wide :], both[:, : 2 * wide])
        pieces[0].append(block[:, :wide])
        pieces[1].append(block[:, wide:])
    for part in range(2):
        out[part] = jnp.concatenate(pieces[part], axis=1)


def solution(mesh):
    chips = mesh.shape["band"] // 2
    owners = mesh.shape["ga"]
    strides = ladder(mesh)

    def per_device(psi, hx):
        parts, rows, depth = psi.shape
        vectors = hx.shape[1]
        height = rows // owners
        width = depth // 2 // CHUNKS
        mid = chips // 2
        lanes = 8 * vectors
        dma = pltpu.SemaphoreType.DMA
        result, _, _ = pl.pallas_call(
            functools.partial(kernel, chips, owners, strides),
            out_shape=(
                jax.ShapeDtypeStruct((parts, height, 2 * vectors * chips), jnp.float32),
                jax.ShapeDtypeStruct((chips - 1, *hx.shape), jnp.float32),
                jax.ShapeDtypeStruct((chips, *hx.shape), jnp.float32),
            ),
            in_specs=[pl.BlockSpec(memory_space=pl.ANY)] * 2,
            out_specs=(
                pl.BlockSpec(memory_space=pltpu.VMEM),
                pl.BlockSpec(memory_space=pl.ANY),
                pl.BlockSpec(memory_space=pl.ANY),
            ),
            scratch_shapes=[
                pltpu.VMEM((SLOTS, 2, parts, rows, width), jnp.float32),
                pltpu.VMEM((SLOTS, 2, parts, 2, vectors, width), jnp.float32),
                pltpu.VMEM((chips, rows, lanes), jnp.float32),
                pltpu.VMEM((mid, rows, lanes), jnp.float32),
                pltpu.VMEM((mid, owners - 1, height, lanes), jnp.float32),
                dma((2, chips - 1, CHUNKS)),
                dma((2, chips - 1, CHUNKS)),
                dma((2, chips, CHUNKS)),
                dma((2, chips, CHUNKS)),
                dma((SLOTS, 2)),
                dma((SLOTS, 2)),
                dma((SLOTS, 2)),
                dma((mid, owners - 1)),
                dma((mid, owners - 1)),
            ],
            compiler_params=pltpu.CompilerParams(
                collective_id=0, has_side_effects=True, vmem_limit_bytes=60 * 2**20
            ),
        )(psi, hx)
        return result

    return jax.shard_map(
        per_device,
        mesh=mesh,
        in_specs=(P(None, "band", "ga"), P(None, "band", "ga")),
        out_specs=P(None, ("band", "ga"), None),
        check_vma=False,
    )
```

```python
import functools

import jax
import jax.numpy as jnp
from jax import lax
from jax.experimental import pallas as pl
from jax.experimental.pallas import tpu as pltpu
from jax.sharding import PartitionSpec as P

CHUNKS = 8
TILE = 512
SLOTS = 3
LAG = 19
WIDE = 2048
MESH = pl.DeviceIdType.MESH


def ladder(mesh):
    chips = mesh.shape["band"] // 2
    try:
        coords = [tuple(mesh.devices[2 * j, 0].coords) for j in range(chips)]
    except AttributeError:
        return 1, 2
    axis = [a != b for a, b in zip(coords[0], coords[1])].index(True)
    if len({c[axis] for c in coords}) == 2:
        return 1, 2
    return chips // 2, 1


def split(x):
    high = x.astype(jnp.bfloat16)
    low = (x - high.astype(jnp.float32)).astype(jnp.bfloat16)
    return high, low


def kernel(
    chips,
    owners,
    strides,
    psi,
    hx,
    out,
    ring,
    twin,
    psi_v,
    hx_v,
    acc,
    final,
    others,
    ring_send,
    ring_recv,
    twin_send,
    twin_recv,
    psi_sem,
    own_sem,
    twin_sem,
    y_send,
    y_recv,
):
    depth = hx.shape[-1]
    half = depth // 2
    width = half // CHUNKS
    rows = psi.shape[1]
    height = rows // owners
    mid = chips // 2
    ticks = chips * CHUNKS
    vectors = hx.shape[1]
    x_stride, z_stride = strides
    long = mid

    me = lax.axis_index("band")
    y = lax.axis_index("ga")
    core = lax.rem(me, 2)
    chip = me // 2
    x = lax.rem(chip // x_stride, 2)
    z = lax.rem(chip // z_stride, long)
    place = z + x * (2 * long - 1 - 2 * z)

    def device_at(position):
        at_x = position // long
        at_z = position + at_x * (2 * long - 1 - 2 * position)
        return 2 * (at_x * x_stride + at_z * z_stride) + core

    after = device_at(lax.rem(place + 1, chips))
    before = device_at(lax.rem(place + chips - 1, chips))
    partner = me + 1 - 2 * core
    target = (after, before)

    def columns(way, c):
        return pl.ds(pl.multiple_of(way * half + c * width, 128), width)

    def with_held(step, way, c, act):
        cols = columns(way, c)
        if isinstance(step, int):
            act(hx.at[:, :, cols] if step == 0 else ring.at[step - 1, :, :, cols])
            return
        pl.when(step == 0)(lambda: act(hx.at[:, :, cols]))
        pl.when(step > 0)(lambda: act(ring.at[step - 1, :, :, cols]))

    def ring_copy(step, way, c, source):
        return pltpu.make_async_remote_copy(
            src_ref=source,
            dst_ref=ring.at[step, :, :, columns(way, c)],
            send_sem=ring_send.at[way, step, c],
            recv_sem=ring_recv.at[way, step, c],
            device_id={"band": target[way]},
            device_id_type=MESH,
        )

    def twin_copy(step, way, c, source):
        return pltpu.make_async_remote_copy(
            src_ref=source,
            dst_ref=twin.at[step, :, :, columns(way, c)],
            send_sem=twin_send.at[way, step, c],
            recv_sem=twin_recv.at[way, step, c],
            device_id={"band": partner},
            device_id_type=MESH,
        )

    def psi_load(t, way):
        c = lax.rem(t, CHUNKS)
        slot = lax.rem(t, SLOTS)
        return pltpu.make_async_copy(
            psi.at[:, :, columns(way, c)], psi_v.at[slot, way], psi_sem.at[slot, way]
        )

    def own_load(t, way, source):
        slot = lax.rem(t, SLOTS)
        return pltpu.make_async_copy(
            source, hx_v.at[slot, way, :, core], own_sem.at[slot, way]
        )

    def twin_load(t, way):
        step, c = t // CHUNKS, lax.rem(t, CHUNKS)
        slot = lax.rem(t, SLOTS)
        return pltpu.make_async_copy(
            twin.at[step, :, :, columns(way, c)],
            hx_v.at[slot, way, :, 1 - core],
            twin_sem.at[slot, way],
        )

    def place_of(step, way):
        late = step // mid
        pair = (1 - late) * step + late * lax.rem(chips - step, mid)
        side = late if way == 0 else lax.rem((step + mid - 1) // mid, 2)
        return 2 * pair + side

    def compute(t, way):
        step, c = t // CHUNKS, lax.rem(t, CHUNKS)
        slot = lax.rem(t, SLOTS)
        own_load(t, way, hx.at[:, :, columns(way, c)]).wait()
        twin_load(t, way).wait()
        psi_load(t, way).wait()
        where = place_of(step, way)
        tile = min(TILE, width)

        def body(k, carry):
            cols = pl.ds(pl.multiple_of(k * tile, 128), tile)
            real = hx_v[slot, way, 0, :, :, cols].reshape(2 * vectors, tile)
            imag = hx_v[slot, way, 1, :, :, cols].reshape(2 * vectors, tile)
            real_high, real_low = split(real)
            imag_high, imag_low = split(imag)
            first = jnp.concatenate([real_high, imag_high, real_low, imag_low], axis=0)
            second = jnp.concatenate(
                [imag_high, -real_high, imag_low, -real_low], axis=0
            )
            total = acc[where]
            for part, right in ((0, first), (1, second)):
                for left in split(psi_v[slot, way, part, :, cols]):
                    total += lax.dot_general(
                        left,
                        right,
                        (((1,), (1,)), ((), ())),
                        preferred_element_type=jnp.float32,
                    )
            acc[where] = total
            return carry

        lax.fori_loop(0, width // tile, body, 0)

    def y_copy(pair, step):
        to = lax.rem(y + step, owners)
        start = pl.multiple_of(to * height, 8)
        return pltpu.make_async_remote_copy(
            src_ref=final.at[pair, pl.ds(start, height)],
            dst_ref=others.at[pair, step - 1],
            send_sem=y_send.at[pair, step - 1],
            recv_sem=y_recv.at[pair, step - 1],
            device_id={"ga": to},
            device_id_type=MESH,
        )

    def finish(step):
        pair = lax.rem(chips - step, mid)
        sides = []
        for side in range(2):
            value = acc[2 * pair + side]
            sides.append(value[:, : 4 * vectors] + value[:, 4 * vectors :])
        final[pair] = jnp.concatenate(sides, axis=1)
        for step_y in range(1, owners):
            y_copy(pair, step_y).start()

    barrier = pltpu.get_barrier_semaphore()
    for neighbour in (after, before, partner):
        pl.semaphore_signal(
            barrier, inc=1, device_id={"band": neighbour}, device_id_type=MESH
        )
    for step_y in range(1, owners):
        pl.semaphore_signal(
            barrier,
            inc=1,
            device_id={"ga": lax.rem(y + step_y, owners)},
            device_id_type=MESH,
        )
    pl.semaphore_wait(barrier, 2 + owners)

    def first_sends(c, carry):
        for way in range(2):
            ring_copy(0, way, c, hx.at[:, :, columns(way, c)]).start()
        return carry

    lax.fori_loop(0, CHUNKS, first_sends, 0)
    acc[...] = jnp.zeros_like(acc)

    def tick(t, carry):
        step, c = t // CHUNKS, lax.rem(t, CHUNKS)

        @pl.when(t < ticks)
        def _():
            for way in range(2):
                psi_load(t, way).start()

        @pl.when(t >= 2)
        def _():
            compute(t - 2, 0)

        @pl.when((t >= 1) & (t <= ticks))
        def _():
            held = t - 1
            held_step, held_c = held // CHUNKS, lax.rem(held, CHUNKS)
            for way in range(2):
                source = hx.at[:, :, columns(way, held_c)]
                twin_copy(held_step, way, held_c, source).wait_recv()
                twin_load(held, way).start()

        @pl.when(t >= 2)
        def _():
            compute(t - 2, 1)
            done = t - 2
            done_step = done // CHUNKS
            pl.when((lax.rem(done, CHUNKS) == CHUNKS - 1) & (done_step >= mid))(
                lambda: finish(done_step)
            )

        @pl.when(t < ticks)
        def _():
            for way in range(2):

                @pl.when(step >= 1)
                def _():
                    source = hx.at[:, :, columns(way, c)]
                    ring_copy(step - 1, way, c, source).wait_recv()

                    @pl.when(step < chips - 1)
                    def _():
                        held = ring.at[step - 1, :, :, columns(way, c)]
                        ring_copy(step, way, c, held).start()

                with_held(
                    step, way, c, lambda ref: twin_copy(step, way, c, ref).start()
                )
                with_held(step, way, c, lambda ref: own_load(t, way, ref).start())

        return carry

    lax.fori_loop(0, ticks + 2, tick, 0)

    def last_waits(t, carry):
        step, c = t // CHUNKS, lax.rem(t, CHUNKS)
        for way in range(2):
            source = hx.at[:, :, columns(way, c)]
            twin_copy(step, way, c, source).wait_send()

            @pl.when(step < chips - 1)
            def _():
                ring_copy(step, way, c, source).wait_send()

        return carry

    lax.fori_loop(0, ticks, last_waits, 0)

    mine = pl.ds(pl.multiple_of(y * height, 8), height)
    for pair in range(mid):
        for step_y in range(1, owners):
            y_copy(pair, step_y).wait_recv()
            final[pair, mine] += others[pair, step_y - 1]
        for step_y in range(1, owners):
            y_copy(pair, step_y).wait_send()

    wide = 2 * vectors
    pieces = [[], []]
    for j in range(chips):
        at_x, at_z = (j // x_stride) % 2, (j // z_stride) % long
        position = at_z + at_x * (2 * long - 1 - 2 * at_z)
        away = lax.rem(place + chips - position, chips)
        late = away // mid
        pair = (1 - late) * away + late * lax.rem(chips - away, mid)
        both = final[pair, mine]
        block = jnp.where(late == 1, both[:, 2 * wide :], both[:, : 2 * wide])
        pieces[0].append(block[:, :wide])
        pieces[1].append(block[:, wide:])
    for part in range(2):
        out[part] = jnp.concatenate(pieces[part], axis=1)


def square_kernel(
    strides,
    psi,
    hx,
    out,
    land,
    twin,
    lent,
    psi_v,
    hx_v,
    acc,
    final,
    others,
    lent_v,
    lent_acc,
    lent_out,
    lent_in,
    got,
    twin_got,
    side_sent,
    end_sent,
    twin_sent,
    load_sem,
    lent_load,
    lent_sent,
    lent_got,
    back_sent,
    back_got,
    y_sent,
    y_got,
):
    width = hx.shape[-1] // 16
    vectors = hx.shape[1]
    rows = psi.shape[1]
    height = rows // 2
    piece = height // 2
    tile = min(WIDE, width)
    x_stride, z_stride = strides

    me = lax.axis_index("band")
    y = lax.axis_index("ga")
    core = lax.rem(me, 2)
    chip = me // 2
    x = lax.rem(chip // x_stride, 2)
    z = lax.rem(chip // z_stride, 4)
    far = z // 2
    node = 3 * far + x * (1 - 2 * far)
    end = lax.rem((z + 1) // 2 + 1, 2)
    odd = lax.rem(node, 2)
    sign = 1 - 2 * odd
    mate = lax.rem(node + sign + 4, 4)
    across = lax.rem(node - sign + 4, 4)
    partner = me + 1 - 2 * core

    def device_at(at, kind):
        at_far = at // 2
        at_x = lax.rem((at + 1) // 2, 2)
        at_z = (1 - kind) * (1 + at_far) + kind * 3 * at_far
        return 2 * (at_x * x_stride + at_z * z_stride) + core

    inner_mate, inner_across = device_at(mate, 0), device_at(across, 0)
    end_mate, own_end, own_inner = device_at(mate, 1), device_at(node, 1), device_at(node, 0)
    inner, outer = end == 0, end == 1
    mine = 2 * node + end

    def columns(g):
        return pl.ds(pl.multiple_of(g * width, 128), width)

    def piece_of(q, way):
        return 2 * q + lax.rem(way + odd, 2)

    def node_at(way, d):
        return lax.rem(node + (2 * way - 1) * sign * d + 12, 4)

    def remote(source, to, dst, send, recv):
        return pltpu.make_async_remote_copy(
            src_ref=source,
            dst_ref=dst,
            send_sem=send,
            recv_sem=recv,
            device_id={"band": to, "ga": y},
            device_id_type=MESH,
        )

    def block_copy(source, src, g, to, send):
        return remote(
            source, to, land.at[src, :, :, columns(g)], send.at[src, g], got.at[src, g]
        )

    def twin_copy(source, src, g):
        return remote(
            source,
            partner,
            twin.at[src, :, :, columns(g)],
            twin_sent.at[src, g],
            twin_got.at[src, g],
        )

    def distance(way, kind, block):
        return lax.rem(block + 5 - kind - (end if way == 0 else 0), 4)

    def unit(t, pos):
        way = 0 if isinstance(pos, int) and pos == 0 else 1
        index = t
        if way:
            index = (1 - end) * t + end * (2 * (t - LAG) + pos - 1)
        block, q = index // 8, lax.rem(index, 8)
        valid = (index >= 0) & (index < 32) & (inner | (q >= 1))
        if way:
            valid &= outer | (pos == 1)
        return way, q, (distance(way, 0, block), distance(way, 1, block)), valid

    def own_of(kind, d):
        return (end == kind) & (d == 0)

    def start_or_end(copy, begin):
        copy.start() if begin else copy.wait_send()

    def pass_one(way, index, kind, valid, begin):
        block, q = index // 8, lax.rem(index, 8)
        d = distance(way, kind, block)
        g = piece_of(q, way)
        src = 2 * node_at(way, d) + kind

        @pl.when(valid & (inner | (q >= 1)) & jnp.logical_not(own_of(kind, d)))
        def _():
            held = land.at[src, :, :, columns(g)]
            if begin:
                block_copy(held, src, g, own_inner, side_sent).wait_recv()

            def send(to, semaphore):
                start_or_end(block_copy(held, src, g, to, semaphore), begin)

            down = (q >= 1) if way == 0 else (q == 1)
            sideways = outer & (q >= 2)
            if kind == 1:
                down &= (d >= 1 + way) & (d <= 2 + way)
                sideways &= d < 3
            onward = inner_mate if way == 0 else inner_across
            pl.when(inner & (d < 3))(lambda: send(onward, side_sent))
            pl.when(inner & down)(lambda: send(own_end, end_sent))
            if way == 0:
                pl.when(sideways)(lambda: send(end_mate, side_sent))
            start_or_end(twin_copy(held, src, g), begin)

    def pass_on(t, begin):
        in_step, end_step, end_late = (t + 28) // 32, (t + 16) // 32, (t + 12) // 32
        for_inner = 2 * t + in_step * (4 - t)
        for_end = t + end_step * (t - 16) + end_late * (20 - t)
        first = (1 - end) * for_inner + end * for_end
        second = 2 * t + 1 - 16 * end
        two = (inner & (t < 4)) | (outer & (t >= 16) & (t < 20))
        for way in range(2):
            fits = inner if way else True
            pass_one(way, first, 0, (t < 20 + 8 * end) & fits, begin)
            pass_one(way, second, 0, two & fits, begin)
        for way in range(2):
            fits = inner if way else True
            pass_one(way, t, 1, (t < 32) & fits, begin)
        for pos in range(2):
            index = 2 * (t - LAG) + pos
            for kind in range(2):
                pass_one(1, index, kind, outer & (index >= 0) & (index < 32), begin)

    def owner_of(k):
        own = k // 2
        return (1 - own) * (1 - y) + own * y

    def lend(k):
        begin = pl.multiple_of(owner_of(k) * height + lax.rem(k, 2) * piece, 8)
        return remote(
            psi.at[:, pl.ds(begin, piece), pl.ds(0, 2 * width)],
            own_inner,
            lent.at[k],
            lent_sent.at[k],
            lent_got.at[k],
        )

    def opening(begin):
        def one(q, carry):
            for way in range(2):
                g = piece_of(q, way)
                source = hx.at[:, :, columns(g)]

                @pl.when(inner)
                def _():
                    to = inner_mate if way == 0 else inner_across
                    start_or_end(block_copy(source, mine, g, to, side_sent), begin)
                    pl.when((q >= 1) if way == 0 else (q == 1))(
                        lambda: start_or_end(
                            block_copy(source, mine, g, own_end, end_sent), begin
                        )
                    )

                @pl.when(outer)
                def _():
                    start_or_end(block_copy(source, mine, g, own_inner, end_sent), begin)
                    pl.when(q >= 1)(
                        lambda: start_or_end(
                            block_copy(source, mine, g, end_mate, side_sent), begin
                        )
                    )

                pl.when(inner | (q >= 1))(
                    lambda: start_or_end(twin_copy(source, mine, g), begin)
                )
            return carry

        lax.fori_loop(0, 8, one, 0)

        @pl.when(outer)
        def _():
            for k in range(4):
                start_or_end(lend(jnp.int32(k)), begin)

    def hx_loads(dst, sems, src, g, kind, own, act):
        cols = columns(g)
        target = dst.at[kind, :, core]
        if act == "wait":
            pltpu.make_async_copy(hx.at[:, :, cols], target, sems.at[2 * kind]).wait()
        else:
            pl.when(own)(
                lambda: pltpu.make_async_copy(
                    hx.at[:, :, cols], target, sems.at[2 * kind]
                ).start()
            )
            pl.when(jnp.logical_not(own))(
                lambda: pltpu.make_async_copy(
                    land.at[src, :, :, cols], target, sems.at[2 * kind]
                ).start()
            )
        other = pltpu.make_async_copy(
            twin.at[src, :, :, cols], dst.at[kind, :, 1 - core], sems.at[2 * kind + 1]
        )
        other.wait() if act == "wait" else other.start()

    def loads(t, act):
        slot = lax.rem(t, 2)
        for pos in range(3):
            way, q, distances, valid = unit(t, pos)
            g = piece_of(q, way)

            @pl.when(valid)
            def _(pos=pos, way=way, distances=distances, g=g):
                sems = load_sem.at[slot, pos]
                weights = pltpu.make_async_copy(
                    psi.at[:, :, columns(g)], psi_v.at[slot, pos], sems.at[4]
                )
                weights.start()
                for kind in range(2):
                    src = 2 * node_at(way, distances[kind]) + kind
                    source = hx.at[:, :, columns(g)]
                    twin_copy(source, src, g).wait_recv()
                    own = own_of(kind, distances[kind])
                    hx_loads(hx_v.at[slot, pos], sems, src, g, kind, own, act)

    def multiply(left_ref, right_ref, total_ref, first_at, second_at):
        def body(k, carry):
            cols = pl.ds(pl.multiple_of(k * tile, 128), tile)
            first, second = [], []
            for kind in range(2):
                real = right_ref[kind, 0, :, :, cols].reshape(2 * vectors, tile)
                imag = right_ref[kind, 1, :, :, cols].reshape(2 * vectors, tile)
                real_high, real_low = split(real)
                imag_high, imag_low = split(imag)
                first += [real_high, imag_high, real_low, imag_low]
                second += [imag_high, -real_high, imag_low, -real_low]
            total = None
            for part, right in ((0, first), (1, second)):
                left = jnp.concatenate(split(left_ref[part, :, cols]), axis=0)
                term = lax.dot_general(
                    left,
                    jnp.concatenate(right, axis=0),
                    (((1,), (1,)), ((), ())),
                    preferred_element_type=jnp.float32,
                )
                total = term if total is None else total + term
            high = total.shape[0] // 2
            total = total[:high] + total[high:]
            lanes = 8 * vectors
            total_ref[first_at] += total[:, :lanes]
            total_ref[second_at] += total[:, lanes:]
            return carry

        if width == tile:
            body(0, 0)
        else:
            lax.fori_loop(0, width // tile, body, 0)

    def compute(t, pos):
        slot = lax.rem(t, 2)
        way, q, distances, valid = unit(t, pos)
        g = piece_of(q, way)

        @pl.when(valid)
        def _():
            sems = load_sem.at[slot, pos]
            pltpu.make_async_copy(
                psi.at[:, :, columns(g)], psi_v.at[slot, pos], sems.at[4]
            ).wait()
            at = []
            for kind in range(2):
                src = 2 * node_at(way, distances[kind]) + kind
                hx_loads(hx_v.at[slot, pos], sems, src, g, kind, None, "wait")
                at.append(src)
            multiply(psi_v.at[slot, pos], hx_v.at[slot, pos], acc, at[0], at[1])

    def fold(value):
        half = 4 * vectors
        return value[:, :half] + value[:, half:]

    def back(k):
        return pltpu.make_async_remote_copy(
            src_ref=lent_out.at[k],
            dst_ref=lent_in.at[k],
            send_sem=back_sent.at[k],
            recv_sem=back_got.at[k],
            device_id={"band": own_end, "ga": owner_of(k)},
            device_id_type=MESH,
        )

    def serve(k, begin, stop):
        pl.when(begin == 0)(lambda: lend(k).wait_recv())

        def places(v):
            way, block = lax.rem(v, 2), v // 2
            return [
                (2 * node_at(way, d) + kind, own_of(kind, d))
                for kind, d in ((0, lax.rem(block + 1, 4)), (1, block))
            ]

        def fetch(v, act):
            g, slot = piece_of(0, lax.rem(v, 2)), lax.rem(v, 2)
            sems = lent_load.at[slot]
            weights = pltpu.make_async_copy(
                lent.at[k, :, :, columns(g)], lent_v.at[slot], sems.at[4]
            )
            weights.wait() if act == "wait" else weights.start()
            for kind, (src, own) in enumerate(places(v)):
                hx_loads(hx_v.at[slot, 2], sems, src, g, kind, own, act)

        fetch(begin, "start")

        def one(v, carry):
            pl.when(v + 1 < stop)(lambda: fetch(v + 1, "start"))
            fetch(v, "wait")
            slot = lax.rem(v, 2)
            (first, _), (second, _) = places(v)
            multiply(
                lent_v.at[slot], hx_v.at[slot, 2], lent_acc.at[k], first, second
            )
            return carry

        lax.fori_loop(begin, stop, one, 0)

        @pl.when(stop == 8)
        def _():
            for at in range(4):
                lent_out[k, at] = jnp.concatenate(
                    [fold(lent_acc[k, 2 * at]), fold(lent_acc[k, 2 * at + 1])], axis=1
                )
            back(k).start()

    barrier = pltpu.get_barrier_semaphore()

    def greet(to, at_y):
        pl.semaphore_signal(
            barrier, inc=1, device_id={"band": to, "ga": at_y}, device_id_type=MESH
        )

    greet(partner, y)
    greet(me, 1 - y)

    @pl.when(inner)
    def _():
        for to in (inner_mate, inner_across, own_end):
            greet(to, y)
        greet(own_end, 1 - y)
        pl.semaphore_wait(barrier, 6)

    @pl.when(outer)
    def _():
        for to in (end_mate, own_inner):
            greet(to, y)
        greet(own_inner, 1 - y)
        pl.semaphore_wait(barrier, 5)

    opening(True)
    acc[...] = jnp.zeros_like(acc)
    lent_acc[...] = jnp.zeros_like(lent_acc)

    def tick(t, carry):
        pl.when(t >= 2)(lambda: compute(t - 2, 0))
        pl.when(t >= 1)(lambda: loads(t - 1, "start"))

        def later(pos, carry):
            compute(t - 2, pos)
            return carry

        @pl.when(t >= 2)
        def _():
            lax.fori_loop(1, 3, later, 0)

        pass_on(t, True)

        early = (t == 18) | (t == 21) | (t == 24)
        late = (t >= 26) & (t < 29)
        last = t == 34
        k = jnp.where(early, (t - 18) // 3, jnp.where(late, t - 26, 3))
        begin = jnp.where(late, 6, 0)
        stop = jnp.where(early, 6, 8)
        pl.when(inner & (early | late | last))(lambda: serve(k, begin, stop))
        return carry

    lax.fori_loop(0, 18 + LAG, tick, 0)

    for at in range(4):
        final[at] = jnp.concatenate([fold(acc[2 * at]), fold(acc[2 * at + 1])], axis=1)

    theirs = pl.ds(pl.multiple_of((1 - y) * height, 8), height)
    ours = pl.ds(pl.multiple_of(y * height, 8), height)

    def y_copy(at):
        return pltpu.make_async_remote_copy(
            src_ref=final.at[at, theirs],
            dst_ref=others.at[at],
            send_sem=y_sent.at[at],
            recv_sem=y_got.at[at],
            device_id={"band": me, "ga": 1 - y},
            device_id_type=MESH,
        )

    for at in range(4):
        y_copy(at).start()

    opening(False)

    def closing(t, carry):
        pass_on(t, False)
        return carry

    lax.fori_loop(0, 16 + LAG, closing, 0)
    for at in range(4):
        y_copy(at).wait_recv()
        final[at, ours] += others[at]

    @pl.when(outer)
    def _():
        for k in range(4):
            back(jnp.int32(k)).wait_recv()
            start = pl.multiple_of(y * height + (k % 2) * piece, 8)
            for at in range(4):
                final[at, pl.ds(start, piece)] += lent_in[k, at]

    for part in range(2):
        pieces = []
        for j in range(8):
            at_x, at_z = (j // x_stride) % 2, (j // z_stride) % 4
            at_far, kind = at_z // 2, ((at_z + 1) // 2 + 1) % 2
            at = 3 * at_far + at_x * (1 - 2 * at_far)
            begin = (2 * kind + part) * 2 * vectors
            pieces.append(final[at, ours][:, begin : begin + 2 * vectors])
        out[part] = jnp.concatenate(pieces, axis=1)
    for at in range(4):
        y_copy(at).wait_send()

    @pl.when(inner)
    def _():
        for k in range(4):
            back(jnp.int32(k)).wait_send()


def solution(mesh):
    chips = mesh.shape["band"] // 2
    owners = mesh.shape["ga"]
    strides = ladder(mesh)

    def by_square(psi, hx):
        parts, rows, depth = psi.shape
        vectors = hx.shape[1]
        height = rows // 2
        width = depth // 16
        lanes = 8 * vectors
        dma = pltpu.SemaphoreType.DMA
        whole = pl.BlockSpec(memory_space=pl.ANY)
        lent = (4, parts, height // 2, 2 * width)
        result, *_ = pl.pallas_call(
            functools.partial(square_kernel, strides),
            out_shape=(
                jax.ShapeDtypeStruct((parts, height, 16 * vectors), jnp.float32),
                jax.ShapeDtypeStruct((8, *hx.shape), jnp.float32),
                jax.ShapeDtypeStruct((8, *hx.shape), jnp.float32),
                jax.ShapeDtypeStruct(lent, jnp.float32),
            ),
            in_specs=[whole] * 2,
            out_specs=(pl.BlockSpec(memory_space=pltpu.VMEM), whole, whole, whole),
            scratch_shapes=[
                pltpu.VMEM((2, 3, parts, rows, width), jnp.float32),
                pltpu.VMEM((2, 3, 2, parts, 2, vectors, width), jnp.float32),
                pltpu.VMEM((8, rows, lanes), jnp.float32),
                pltpu.VMEM((4, rows, lanes), jnp.float32),
                pltpu.VMEM((4, height, lanes), jnp.float32),
                pltpu.VMEM((2, parts, height // 2, width), jnp.float32),
                pltpu.VMEM((4, 8, height // 2, lanes), jnp.float32),
                pltpu.VMEM((4, 4, height // 2, lanes), jnp.float32),
                pltpu.VMEM((4, 4, height // 2, lanes), jnp.float32),
                *[dma((8, 16))] * 5,
                dma((2, 3, 5)),
                dma((2, 5)),
                *[dma((4,))] * 6,
            ],
            compiler_params=pltpu.CompilerParams(
                collective_id=0, has_side_effects=True, vmem_limit_bytes=60 * 2**20
            ),
        )(psi, hx)
        return result

    def by_ring(psi, hx):
        parts, rows, depth = psi.shape
        vectors = hx.shape[1]
        height = rows // owners
        width = depth // 2 // CHUNKS
        mid = chips // 2
        lanes = 8 * vectors
        dma = pltpu.SemaphoreType.DMA
        result, _, _ = pl.pallas_call(
            functools.partial(kernel, chips, owners, strides),
            out_shape=(
                jax.ShapeDtypeStruct((parts, height, 2 * vectors * chips), jnp.float32),
                jax.ShapeDtypeStruct((chips - 1, *hx.shape), jnp.float32),
                jax.ShapeDtypeStruct((chips, *hx.shape), jnp.float32),
            ),
            in_specs=[pl.BlockSpec(memory_space=pl.ANY)] * 2,
            out_specs=(
                pl.BlockSpec(memory_space=pltpu.VMEM),
                pl.BlockSpec(memory_space=pl.ANY),
                pl.BlockSpec(memory_space=pl.ANY),
            ),
            scratch_shapes=[
                pltpu.VMEM((SLOTS, 2, parts, rows, width), jnp.float32),
                pltpu.VMEM((SLOTS, 2, parts, 2, vectors, width), jnp.float32),
                pltpu.VMEM((chips, rows, lanes), jnp.float32),
                pltpu.VMEM((mid, rows, lanes), jnp.float32),
                pltpu.VMEM((mid, owners - 1, height, lanes), jnp.float32),
                dma((2, chips - 1, CHUNKS)),
                dma((2, chips - 1, CHUNKS)),
                dma((2, chips, CHUNKS)),
                dma((2, chips, CHUNKS)),
                dma((SLOTS, 2)),
                dma((SLOTS, 2)),
                dma((SLOTS, 2)),
                dma((mid, owners - 1)),
                dma((mid, owners - 1)),
            ],
            compiler_params=pltpu.CompilerParams(
                collective_id=0, has_side_effects=True, vmem_limit_bytes=60 * 2**20
            ),
        )(psi, hx)
        return result

    return jax.shard_map(
        by_square if (chips, owners) == (8, 2) else by_ring,
        mesh=mesh,
        in_specs=(P(None, "band", "ga"), P(None, "band", "ga")),
        out_specs=P(None, ("band", "ga"), None),
        check_vma=False,
    )
```

```python
import functools

import jax
import jax.numpy as jnp
from jax import lax
from jax.experimental import pallas as pl
from jax.experimental.pallas import tpu as pltpu
from jax.sharding import PartitionSpec as P

CHUNKS = 8
TILE = 512
SLOTS = 3
LAG = 19
WIDE = 2048
MESH = pl.DeviceIdType.MESH


def ladder(mesh):
    chips = mesh.shape["band"] // 2
    try:
        coords = [tuple(mesh.devices[2 * j, 0].coords) for j in range(chips)]
    except AttributeError:
        return 1, 2
    axis = [a != b for a, b in zip(coords[0], coords[1])].index(True)
    if len({c[axis] for c in coords}) == 2:
        return 1, 2
    return chips // 2, 1


def split(x):
    high = x.astype(jnp.bfloat16)
    low = (x - high.astype(jnp.float32)).astype(jnp.bfloat16)
    return high, low


def kernel(
    chips,
    owners,
    strides,
    psi,
    hx,
    out,
    ring,
    twin,
    psi_v,
    hx_v,
    acc,
    final,
    others,
    ring_send,
    ring_recv,
    twin_send,
    twin_recv,
    psi_sem,
    own_sem,
    twin_sem,
    y_send,
    y_recv,
):
    depth = hx.shape[-1]
    half = depth // 2
    width = half // CHUNKS
    rows = psi.shape[1]
    height = rows // owners
    mid = chips // 2
    ticks = chips * CHUNKS
    vectors = hx.shape[1]
    x_stride, z_stride = strides
    long = mid

    me = lax.axis_index("band")
    y = lax.axis_index("ga")
    core = lax.rem(me, 2)
    chip = me // 2
    x = lax.rem(chip // x_stride, 2)
    z = lax.rem(chip // z_stride, long)
    place = z + x * (2 * long - 1 - 2 * z)

    def device_at(position):
        at_x = position // long
        at_z = position + at_x * (2 * long - 1 - 2 * position)
        return 2 * (at_x * x_stride + at_z * z_stride) + core

    after = device_at(lax.rem(place + 1, chips))
    before = device_at(lax.rem(place + chips - 1, chips))
    partner = me + 1 - 2 * core
    target = (after, before)

    def columns(way, c):
        return pl.ds(pl.multiple_of(way * half + c * width, 128), width)

    def with_held(step, way, c, act):
        cols = columns(way, c)
        if isinstance(step, int):
            act(hx.at[:, :, cols] if step == 0 else ring.at[step - 1, :, :, cols])
            return
        pl.when(step == 0)(lambda: act(hx.at[:, :, cols]))
        pl.when(step > 0)(lambda: act(ring.at[step - 1, :, :, cols]))

    def ring_copy(step, way, c, source):
        return pltpu.make_async_remote_copy(
            src_ref=source,
            dst_ref=ring.at[step, :, :, columns(way, c)],
            send_sem=ring_send.at[way, step, c],
            recv_sem=ring_recv.at[way, step, c],
            device_id={"band": target[way]},
            device_id_type=MESH,
        )

    def twin_copy(step, way, c, source):
        return pltpu.make_async_remote_copy(
            src_ref=source,
            dst_ref=twin.at[step, :, :, columns(way, c)],
            send_sem=twin_send.at[way, step, c],
            recv_sem=twin_recv.at[way, step, c],
            device_id={"band": partner},
            device_id_type=MESH,
        )

    def psi_load(t, way):
        c = lax.rem(t, CHUNKS)
        slot = lax.rem(t, SLOTS)
        return pltpu.make_async_copy(
            psi.at[:, :, columns(way, c)], psi_v.at[slot, way], psi_sem.at[slot, way]
        )

    def own_load(t, way, source):
        slot = lax.rem(t, SLOTS)
        return pltpu.make_async_copy(
            source, hx_v.at[slot, way, :, core], own_sem.at[slot, way]
        )

    def twin_load(t, way):
        step, c = t // CHUNKS, lax.rem(t, CHUNKS)
        slot = lax.rem(t, SLOTS)
        return pltpu.make_async_copy(
            twin.at[step, :, :, columns(way, c)],
            hx_v.at[slot, way, :, 1 - core],
            twin_sem.at[slot, way],
        )

    def place_of(step, way):
        late = step // mid
        pair = (1 - late) * step + late * lax.rem(chips - step, mid)
        side = late if way == 0 else lax.rem((step + mid - 1) // mid, 2)
        return 2 * pair + side

    def compute(t, way):
        step, c = t // CHUNKS, lax.rem(t, CHUNKS)
        slot = lax.rem(t, SLOTS)
        own_load(t, way, hx.at[:, :, columns(way, c)]).wait()
        twin_load(t, way).wait()
        psi_load(t, way).wait()
        where = place_of(step, way)
        tile = min(TILE, width)

        def body(k, carry):
            cols = pl.ds(pl.multiple_of(k * tile, 128), tile)
            real = hx_v[slot, way, 0, :, :, cols].reshape(2 * vectors, tile)
            imag = hx_v[slot, way, 1, :, :, cols].reshape(2 * vectors, tile)
            real_high, real_low = split(real)
            imag_high, imag_low = split(imag)
            first = jnp.concatenate([real_high, imag_high, real_low, imag_low], axis=0)
            second = jnp.concatenate(
                [imag_high, -real_high, imag_low, -real_low], axis=0
            )
            total = acc[where]
            for part, right in ((0, first), (1, second)):
                for left in split(psi_v[slot, way, part, :, cols]):
                    total += lax.dot_general(
                        left,
                        right,
                        (((1,), (1,)), ((), ())),
                        preferred_element_type=jnp.float32,
                    )
            acc[where] = total
            return carry

        lax.fori_loop(0, width // tile, body, 0)

    def y_copy(pair, step):
        to = lax.rem(y + step, owners)
        start = pl.multiple_of(to * height, 8)
        return pltpu.make_async_remote_copy(
            src_ref=final.at[pair, pl.ds(start, height)],
            dst_ref=others.at[pair, step - 1],
            send_sem=y_send.at[pair, step - 1],
            recv_sem=y_recv.at[pair, step - 1],
            device_id={"ga": to},
            device_id_type=MESH,
        )

    def finish(step):
        pair = lax.rem(chips - step, mid)
        sides = []
        for side in range(2):
            value = acc[2 * pair + side]
            sides.append(value[:, : 4 * vectors] + value[:, 4 * vectors :])
        final[pair] = jnp.concatenate(sides, axis=1)
        for step_y in range(1, owners):
            y_copy(pair, step_y).start()

    barrier = pltpu.get_barrier_semaphore()
    for neighbour in (after, before, partner):
        pl.semaphore_signal(
            barrier, inc=1, device_id={"band": neighbour}, device_id_type=MESH
        )
    for step_y in range(1, owners):
        pl.semaphore_signal(
            barrier,
            inc=1,
            device_id={"ga": lax.rem(y + step_y, owners)},
            device_id_type=MESH,
        )
    pl.semaphore_wait(barrier, 2 + owners)

    def first_sends(c, carry):
        for way in range(2):
            ring_copy(0, way, c, hx.at[:, :, columns(way, c)]).start()
        return carry

    lax.fori_loop(0, CHUNKS, first_sends, 0)
    acc[...] = jnp.zeros_like(acc)

    def tick(t, carry):
        step, c = t // CHUNKS, lax.rem(t, CHUNKS)

        @pl.when(t < ticks)
        def _():
            for way in range(2):
                psi_load(t, way).start()

        @pl.when(t >= 2)
        def _():
            compute(t - 2, 0)

        @pl.when((t >= 1) & (t <= ticks))
        def _():
            held = t - 1
            held_step, held_c = held // CHUNKS, lax.rem(held, CHUNKS)
            for way in range(2):
                source = hx.at[:, :, columns(way, held_c)]
                twin_copy(held_step, way, held_c, source).wait_recv()
                twin_load(held, way).start()

        @pl.when(t >= 2)
        def _():
            compute(t - 2, 1)
            done = t - 2
            done_step = done // CHUNKS
            pl.when((lax.rem(done, CHUNKS) == CHUNKS - 1) & (done_step >= mid))(
                lambda: finish(done_step)
            )

        @pl.when(t < ticks)
        def _():
            for way in range(2):

                @pl.when(step >= 1)
                def _():
                    source = hx.at[:, :, columns(way, c)]
                    ring_copy(step - 1, way, c, source).wait_recv()

                    @pl.when(step < chips - 1)
                    def _():
                        held = ring.at[step - 1, :, :, columns(way, c)]
                        ring_copy(step, way, c, held).start()

                with_held(
                    step, way, c, lambda ref: twin_copy(step, way, c, ref).start()
                )
                with_held(step, way, c, lambda ref: own_load(t, way, ref).start())

        return carry

    lax.fori_loop(0, ticks + 2, tick, 0)

    def last_waits(t, carry):
        step, c = t // CHUNKS, lax.rem(t, CHUNKS)
        for way in range(2):
            source = hx.at[:, :, columns(way, c)]
            twin_copy(step, way, c, source).wait_send()

            @pl.when(step < chips - 1)
            def _():
                ring_copy(step, way, c, source).wait_send()

        return carry

    lax.fori_loop(0, ticks, last_waits, 0)

    mine = pl.ds(pl.multiple_of(y * height, 8), height)
    for pair in range(mid):
        for step_y in range(1, owners):
            y_copy(pair, step_y).wait_recv()
            final[pair, mine] += others[pair, step_y - 1]
        for step_y in range(1, owners):
            y_copy(pair, step_y).wait_send()

    wide = 2 * vectors
    pieces = [[], []]
    for j in range(chips):
        at_x, at_z = (j // x_stride) % 2, (j // z_stride) % long
        position = at_z + at_x * (2 * long - 1 - 2 * at_z)
        away = lax.rem(place + chips - position, chips)
        late = away // mid
        pair = (1 - late) * away + late * lax.rem(chips - away, mid)
        both = final[pair, mine]
        block = jnp.where(late == 1, both[:, 2 * wide :], both[:, : 2 * wide])
        pieces[0].append(block[:, :wide])
        pieces[1].append(block[:, wide:])
    for part in range(2):
        out[part] = jnp.concatenate(pieces[part], axis=1)


def square_kernel(
    strides,
    psi,
    hx,
    out,
    land,
    twin,
    lent,
    psi_v,
    hx_v,
    acc,
    final,
    others,
    lent_v,
    lent_hx,
    lent_acc,
    lent_out,
    lent_in,
    got,
    twin_got,
    side_sent,
    end_sent,
    twin_sent,
    load_sem,
    lent_load,
    lent_sent,
    lent_got,
    back_sent,
    back_got,
    y_sent,
    y_got,
):
    width = hx.shape[-1] // 16
    vectors = hx.shape[1]
    rows = psi.shape[1]
    height = rows // 2
    piece = height // 2
    tile = min(WIDE, width)
    x_stride, z_stride = strides

    me = lax.axis_index("band")
    y = lax.axis_index("ga")
    core = lax.rem(me, 2)
    chip = me // 2
    x = lax.rem(chip // x_stride, 2)
    z = lax.rem(chip // z_stride, 4)
    far = z // 2
    node = 3 * far + x * (1 - 2 * far)
    end = lax.rem((z + 1) // 2 + 1, 2)
    odd = lax.rem(node, 2)
    sign = 1 - 2 * odd
    mate = lax.rem(node + sign + 4, 4)
    across = lax.rem(node - sign + 4, 4)
    partner = me + 1 - 2 * core

    def device_at(at, kind):
        at_far = at // 2
        at_x = lax.rem((at + 1) // 2, 2)
        at_z = (1 - kind) * (1 + at_far) + kind * 3 * at_far
        return 2 * (at_x * x_stride + at_z * z_stride) + core

    inner_mate, inner_across = device_at(mate, 0), device_at(across, 0)
    end_mate, own_end, own_inner = device_at(mate, 1), device_at(node, 1), device_at(node, 0)
    inner, outer = end == 0, end == 1
    mine = 2 * node + end

    def columns(g):
        return pl.ds(pl.multiple_of(g * width, 128), width)

    def piece_of(q, way):
        return 2 * q + lax.rem(way + odd, 2)

    def node_at(way, d):
        return lax.rem(node + (2 * way - 1) * sign * d + 12, 4)

    def remote(source, to, dst, send, recv):
        return pltpu.make_async_remote_copy(
            src_ref=source,
            dst_ref=dst,
            send_sem=send,
            recv_sem=recv,
            device_id={"band": to, "ga": y},
            device_id_type=MESH,
        )

    def block_copy(source, src, g, to, send):
        return remote(
            source, to, land.at[src, :, :, columns(g)], send, got.at[src, g]
        )

    def twin_copy(source, src, g):
        return remote(
            source,
            partner,
            twin.at[src, :, :, columns(g)],
            twin_sent,
            twin_got.at[src, g],
        )

    def distance(way, kind, block):
        return lax.rem(block + 5 - kind - (end if way == 0 else 0), 4)

    def unit(t, pos):
        way = 0 if isinstance(pos, int) and pos == 0 else 1
        index = t
        if way:
            index = (1 - end) * t + end * (2 * (t - LAG) + pos - 1)
        block, q = index // 8, lax.rem(index, 8)
        valid = (index >= 0) & (index < 32) & (inner | (q >= 1))
        if way:
            valid &= outer | (pos == 1)
        return way, q, (distance(way, 0, block), distance(way, 1, block)), valid

    def own_of(kind, d):
        return (end == kind) & (d == 0)

    def pass_one(way, index, kind, valid):
        block, q = index // 8, lax.rem(index, 8)
        d = distance(way, kind, block)
        g = piece_of(q, way)
        src = 2 * node_at(way, d) + kind

        @pl.when(valid & (inner | (q >= 1)) & jnp.logical_not(own_of(kind, d)))
        def _():
            held = land.at[src, :, :, columns(g)]
            block_copy(held, src, g, own_inner, side_sent).wait_recv()

            def send(to, semaphore):
                block_copy(held, src, g, to, semaphore).start()

            down = (q >= 1) if way == 0 else (q == 1)
            sideways = outer & (q >= 2)
            if kind == 1:
                down &= (d >= 1 + way) & (d <= 2 + way)
                sideways &= d < 3
            onward = inner_mate if way == 0 else inner_across
            pl.when(inner & (d < 3))(lambda: send(onward, side_sent))
            pl.when(inner & down)(lambda: send(own_end, end_sent))
            if way == 0:
                pl.when(sideways)(lambda: send(end_mate, side_sent))
            twin_copy(held, src, g).start()

    def pass_on(t):
        in_step, end_step, end_late = (t + 28) // 32, (t + 16) // 32, (t + 12) // 32
        for_inner = 2 * t + in_step * (4 - t)
        for_end = t + end_step * (t - 16) + end_late * (20 - t)
        first = (1 - end) * for_inner + end * for_end
        second = 2 * t + 1 - 16 * end
        two = (inner & (t < 4)) | (outer & (t >= 16) & (t < 20))
        for way in range(2):
            fits = inner if way else True
            pass_one(way, first, 0, (t < 20 + 8 * end) & fits)
            pass_one(way, second, 0, two & fits)
        for way in range(2):
            fits = inner if way else True
            pass_one(way, t, 1, (t < 32) & fits)
        for pos in range(2):
            index = 2 * (t - LAG) + pos
            for kind in range(2):
                pass_one(1, index, kind, outer & (index >= 0) & (index < 32))

    def owner_of(k):
        own = k // 2
        return (1 - own) * (1 - y) + own * y

    def lend(k):
        begin = pl.multiple_of(owner_of(k) * height + lax.rem(k, 2) * piece, 8)
        return remote(
            psi.at[:, pl.ds(begin, piece), pl.ds(0, 2 * width)],
            own_inner,
            lent.at[k],
            lent_sent.at[k],
            lent_got.at[k],
        )

    def opening():
        def one(q, carry):
            for way in range(2):
                g = piece_of(q, way)
                source = hx.at[:, :, columns(g)]

                def send(to, semaphore):
                    block_copy(source, mine, g, to, semaphore).start()

                onward = inner_mate if way == 0 else inner_across
                down = (q >= 1) if way == 0 else (q == 1)
                pl.when(inner)(lambda: send(onward, side_sent))
                pl.when(inner & down)(lambda: send(own_end, end_sent))
                pl.when(outer)(lambda: send(own_inner, end_sent))
                pl.when(outer & (q >= 1))(lambda: send(end_mate, side_sent))
                pl.when(inner | (q >= 1))(
                    lambda: twin_copy(source, mine, g).start()
                )
            return carry

        lax.fori_loop(0, 8, one, 0)

        @pl.when(outer)
        def _():
            for k in range(4):
                lend(jnp.int32(k)).start()

    def hx_loads(dst, sems, src, g, kind, own, act):
        cols = columns(g)
        target = dst.at[kind, :, core]
        if act == "wait":
            pltpu.make_async_copy(hx.at[:, :, cols], target, sems.at[2 * kind]).wait()
        else:
            pl.when(own)(
                lambda: pltpu.make_async_copy(
                    hx.at[:, :, cols], target, sems.at[2 * kind]
                ).start()
            )
            pl.when(jnp.logical_not(own))(
                lambda: pltpu.make_async_copy(
                    land.at[src, :, :, cols], target, sems.at[2 * kind]
                ).start()
            )
        other = pltpu.make_async_copy(
            twin.at[src, :, :, cols], dst.at[kind, :, 1 - core], sems.at[2 * kind + 1]
        )
        other.wait() if act == "wait" else other.start()

    def loads(t, act):
        slot = lax.rem(t, 2)
        for pos in range(3):
            way, q, distances, valid = unit(t, pos)
            g = piece_of(q, way)

            @pl.when(valid)
            def _(pos=pos, way=way, distances=distances, g=g):
                sems = load_sem.at[slot, pos]
                weights = pltpu.make_async_copy(
                    psi.at[:, :, columns(g)], psi_v.at[slot, pos], sems.at[4]
                )
                weights.start()
                for kind in range(2):
                    src = 2 * node_at(way, distances[kind]) + kind
                    source = hx.at[:, :, columns(g)]
                    twin_copy(source, src, g).wait_recv()
                    own = own_of(kind, distances[kind])
                    hx_loads(hx_v.at[slot, pos], sems, src, g, kind, own, act)

    def multiply(left_ref, right_ref, total_ref, first_at, second_at):
        def body(k, carry):
            cols = pl.ds(pl.multiple_of(k * tile, 128), tile)
            first, second = [], []
            for kind in range(2):
                real = right_ref[kind, 0, :, :, cols].reshape(2 * vectors, tile)
                imag = right_ref[kind, 1, :, :, cols].reshape(2 * vectors, tile)
                real_high, real_low = split(real)
                imag_high, imag_low = split(imag)
                first += [real_high, imag_high, real_low, imag_low]
                second += [imag_high, -real_high, imag_low, -real_low]
            total = None
            for part, right in ((0, first), (1, second)):
                left = jnp.concatenate(split(left_ref[part, :, cols]), axis=0)
                term = lax.dot_general(
                    left,
                    jnp.concatenate(right, axis=0),
                    (((1,), (1,)), ((), ())),
                    preferred_element_type=jnp.float32,
                )
                total = term if total is None else total + term
            high = total.shape[0] // 2
            total = total[:high] + total[high:]
            lanes = 8 * vectors
            total_ref[first_at] += total[:, :lanes]
            total_ref[second_at] += total[:, lanes:]
            return carry

        if width == tile:
            body(0, 0)
        else:
            lax.fori_loop(0, width // tile, body, 0)

    def compute(t, pos):
        slot = lax.rem(t, 2)
        way, q, distances, valid = unit(t, pos)
        g = piece_of(q, way)

        @pl.when(valid)
        def _():
            sems = load_sem.at[slot, pos]
            pltpu.make_async_copy(
                psi.at[:, :, columns(g)], psi_v.at[slot, pos], sems.at[4]
            ).wait()
            at = []
            for kind in range(2):
                src = 2 * node_at(way, distances[kind]) + kind
                hx_loads(hx_v.at[slot, pos], sems, src, g, kind, None, "wait")
                at.append(src)
            multiply(psi_v.at[slot, pos], hx_v.at[slot, pos], acc, at[0], at[1])

    def fold(value):
        half = 4 * vectors
        return value[:, :half] + value[:, half:]

    def back(k):
        return pltpu.make_async_remote_copy(
            src_ref=lent_out.at[k],
            dst_ref=lent_in.at[k],
            send_sem=back_sent.at[k],
            recv_sem=back_got.at[k],
            device_id={"band": own_end, "ga": owner_of(k)},
            device_id_type=MESH,
        )

    def serve(first_k, late, stop):
        pl.when(late == 0)(lambda: lend(first_k).wait_recv())

        def job(u):
            return first_k + late * (u // 2), u + late * (6 - 2 * (u // 2))

        def places(v):
            way, block = lax.rem(v, 2), v // 2
            return [
                (2 * node_at(way, d) + kind, own_of(kind, d))
                for kind, d in ((0, lax.rem(block + 1, 4)), (1, block))
            ]

        def fetch(u, act):
            k, v = job(u)
            g, slot = piece_of(0, lax.rem(v, 2)), lax.rem(u, 3)
            sems = lent_load.at[slot]
            weights = pltpu.make_async_copy(
                lent.at[k, :, :, columns(g)], lent_v.at[slot], sems.at[4]
            )
            weights.wait() if act == "wait" else weights.start()
            for kind, (src, own) in enumerate(places(v)):
                hx_loads(lent_hx.at[slot], sems, src, g, kind, own, act)

        fetch(jnp.int32(0), "start")
        fetch(jnp.int32(1), "start")

        def one(u, carry):
            pl.when(u + 2 < stop)(lambda: fetch(u + 2, "start"))
            fetch(u, "wait")
            k, v = job(u)
            slot = lax.rem(u, 3)
            (first, _), (second, _) = places(v)
            multiply(lent_v.at[slot], lent_hx.at[slot], lent_acc.at[k], first, second)
            return carry

        lax.fori_loop(0, stop, one, 0)

        def give(k):
            for at in range(4):
                lent_out[k, at] = jnp.concatenate(
                    [fold(lent_acc[k, 2 * at]), fold(lent_acc[k, 2 * at + 1])], axis=1
                )
            back(jnp.int32(k)).start()

        @pl.when(late == 1)
        def _():
            for k in range(3):
                give(k)

        pl.when(stop == 8)(lambda: give(3))

    barrier = pltpu.get_barrier_semaphore()

    def greet(to, at_y):
        pl.semaphore_signal(
            barrier, inc=1, device_id={"band": to, "ga": at_y}, device_id_type=MESH
        )

    greet(partner, y)
    greet(me, 1 - y)

    @pl.when(inner)
    def _():
        for to in (inner_mate, inner_across, own_end):
            greet(to, y)
        greet(own_end, 1 - y)
        pl.semaphore_wait(barrier, 6)

    @pl.when(outer)
    def _():
        for to in (end_mate, own_inner):
            greet(to, y)
        greet(own_inner, 1 - y)
        pl.semaphore_wait(barrier, 5)

    opening()
    acc[...] = jnp.zeros_like(acc)
    lent_acc[...] = jnp.zeros_like(lent_acc)

    def tick(t, carry):
        pl.when(t >= 2)(lambda: compute(t - 2, 0))
        pl.when(t >= 1)(lambda: loads(t - 1, "start"))

        def later(pos, carry):
            compute(t - 2, pos)
            return carry

        @pl.when(t >= 2)
        def _():
            lax.fori_loop(1, 3, later, 0)

        pass_on(t)

        early = (t == 17) | (t == 18) | (t == 23)
        late = jnp.where(t == 26, 1, 0)
        last = t == 34
        k = jnp.where(early, (t - 16) // 3 + t // 18 - t // 23, 3 - 3 * late)
        stop = jnp.where(last, 8, 6)
        pl.when(inner & (early | (t == 26) | last))(lambda: serve(k, late, stop))
        return carry

    lax.fori_loop(0, 18 + LAG, tick, 0)

    for at in range(4):
        final[at] = jnp.concatenate([fold(acc[2 * at]), fold(acc[2 * at + 1])], axis=1)

    theirs = pl.ds(pl.multiple_of((1 - y) * height, 8), height)
    ours = pl.ds(pl.multiple_of(y * height, 8), height)

    def y_copy(at):
        return pltpu.make_async_remote_copy(
            src_ref=final.at[at, theirs],
            dst_ref=others.at[at],
            send_sem=y_sent.at[at],
            recv_sem=y_got.at[at],
            device_id={"band": me, "ga": 1 - y},
            device_id_type=MESH,
        )

    for at in range(4):
        y_copy(at).start()

    def sent(semaphore, *refs):
        for ref in refs:
            pltpu.make_async_copy(ref, ref, semaphore).wait()

    @pl.when(inner)
    def _():
        sent(side_sent, land.at[pl.ds(0, 6)])
        sent(end_sent, land.at[pl.ds(0, 3)])
        sent(twin_sent, land)

    @pl.when(outer)
    def _():
        sent(side_sent, land.at[pl.ds(0, 3)], land.at[0, :, :, pl.ds(0, 2 * width)])
        sent(end_sent, land.at[0])
        sent(twin_sent, land.at[pl.ds(0, 7)])
        for k in range(4):
            lend(jnp.int32(k)).wait_send()

    for at in range(4):
        y_copy(at).wait_recv()
        final[at, ours] += others[at]

    @pl.when(outer)
    def _():
        for k in range(4):
            back(jnp.int32(k)).wait_recv()
            start = pl.multiple_of(y * height + (k % 2) * piece, 8)
            for at in range(4):
                final[at, pl.ds(start, piece)] += lent_in[k, at]

    for part in range(2):
        pieces = []
        for j in range(8):
            at_x, at_z = (j // x_stride) % 2, (j // z_stride) % 4
            at_far, kind = at_z // 2, ((at_z + 1) // 2 + 1) % 2
            at = 3 * at_far + at_x * (1 - 2 * at_far)
            begin = (2 * kind + part) * 2 * vectors
            pieces.append(final[at, ours][:, begin : begin + 2 * vectors])
        out[part] = jnp.concatenate(pieces, axis=1)
    for at in range(4):
        y_copy(at).wait_send()

    @pl.when(inner)
    def _():
        for k in range(4):
            back(jnp.int32(k)).wait_send()


def solution(mesh):
    chips = mesh.shape["band"] // 2
    owners = mesh.shape["ga"]
    strides = ladder(mesh)

    def by_square(psi, hx):
        parts, rows, depth = psi.shape
        vectors = hx.shape[1]
        height = rows // 2
        width = depth // 16
        lanes = 8 * vectors
        dma = pltpu.SemaphoreType.DMA
        whole = pl.BlockSpec(memory_space=pl.ANY)
        lent = (4, parts, height // 2, 2 * width)
        result, *_ = pl.pallas_call(
            functools.partial(square_kernel, strides),
            out_shape=(
                jax.ShapeDtypeStruct((parts, height, 16 * vectors), jnp.float32),
                jax.ShapeDtypeStruct((8, *hx.shape), jnp.float32),
                jax.ShapeDtypeStruct((8, *hx.shape), jnp.float32),
                jax.ShapeDtypeStruct(lent, jnp.float32),
            ),
            in_specs=[whole] * 2,
            out_specs=(pl.BlockSpec(memory_space=pltpu.VMEM), whole, whole, whole),
            scratch_shapes=[
                pltpu.VMEM((2, 3, parts, rows, width), jnp.float32),
                pltpu.VMEM((2, 3, 2, parts, 2, vectors, width), jnp.float32),
                pltpu.VMEM((8, rows, lanes), jnp.float32),
                pltpu.VMEM((4, rows, lanes), jnp.float32),
                pltpu.VMEM((4, height, lanes), jnp.float32),
                pltpu.VMEM((3, parts, height // 2, width), jnp.float32),
                pltpu.VMEM((3, 2, parts, 2, vectors, width), jnp.float32),
                pltpu.VMEM((4, 8, height // 2, lanes), jnp.float32),
                pltpu.VMEM((4, 4, height // 2, lanes), jnp.float32),
                pltpu.VMEM((4, 4, height // 2, lanes), jnp.float32),
                *[dma((8, 16))] * 2,
                *[dma] * 3,
                dma((2, 3, 5)),
                dma((3, 5)),
                *[dma((4,))] * 6,
            ],
            compiler_params=pltpu.CompilerParams(
                collective_id=0, has_side_effects=True, vmem_limit_bytes=60 * 2**20
            ),
        )(psi, hx)
        return result

    def by_ring(psi, hx):
        parts, rows, depth = psi.shape
        vectors = hx.shape[1]
        height = rows // owners
        width = depth // 2 // CHUNKS
        mid = chips // 2
        lanes = 8 * vectors
        dma = pltpu.SemaphoreType.DMA
        result, _, _ = pl.pallas_call(
            functools.partial(kernel, chips, owners, strides),
            out_shape=(
                jax.ShapeDtypeStruct((parts, height, 2 * vectors * chips), jnp.float32),
                jax.ShapeDtypeStruct((chips - 1, *hx.shape), jnp.float32),
                jax.ShapeDtypeStruct((chips, *hx.shape), jnp.float32),
            ),
            in_specs=[pl.BlockSpec(memory_space=pl.ANY)] * 2,
            out_specs=(
                pl.BlockSpec(memory_space=pltpu.VMEM),
                pl.BlockSpec(memory_space=pl.ANY),
                pl.BlockSpec(memory_space=pl.ANY),
            ),
            scratch_shapes=[
                pltpu.VMEM((SLOTS, 2, parts, rows, width), jnp.float32),
                pltpu.VMEM((SLOTS, 2, parts, 2, vectors, width), jnp.float32),
                pltpu.VMEM((chips, rows, lanes), jnp.float32),
                pltpu.VMEM((mid, rows, lanes), jnp.float32),
                pltpu.VMEM((mid, owners - 1, height, lanes), jnp.float32),
                dma((2, chips - 1, CHUNKS)),
                dma((2, chips - 1, CHUNKS)),
                dma((2, chips, CHUNKS)),
                dma((2, chips, CHUNKS)),
                dma((SLOTS, 2)),
                dma((SLOTS, 2)),
                dma((SLOTS, 2)),
                dma((mid, owners - 1)),
                dma((mid, owners - 1)),
            ],
            compiler_params=pltpu.CompilerParams(
                collective_id=0, has_side_effects=True, vmem_limit_bytes=60 * 2**20
            ),
        )(psi, hx)
        return result

    return jax.shard_map(
        by_square if (chips, owners) == (8, 2) else by_ring,
        mesh=mesh,
        in_specs=(P(None, "band", "ga"), P(None, "band", "ga")),
        out_specs=P(None, ("band", "ga"), None),
        check_vma=False,
    )
```
